256 devices in a mesh: expert: 64 (over x, z, core), half: 4 (over y).
Axes of the slice: x: 4, y: 4, z: 8, core: 2. Of those that a mesh axis runs over, the one named last changes fastest.
Arguments:
- tokens: bfloat16 [8192, 2048], P('expert'), may hold values from -6 to 6
- out_grad: bfloat16 [8192, 2048], P('expert'), may hold values from -6 to 6
- assign: int32 [8192, 8], P('expert'), may hold values from 0 to 127, all different within a row; in each aligned block of 128 rows (0 to 127, 128 to 255, ...) at most 12 rows name the same one
- gate_weights: bfloat16 [8192, 8], P('expert'), may hold values from 0.099609375 to 1
- w_gate: bfloat16 [128, 768, 2048], P('expert', 'half'), may hold values from -0.125 to 0.125
- w_up: bfloat16 [128, 768, 2048], P('expert', 'half'), may hold values from -0.125 to 0.125
- w_down: bfloat16 [128, 768, 2048], P('expert', 'half'), may hold values from -0.21875 to 0.21875
Outputs:
- input_grad: bfloat16 [8192, 2048], P(('expert', 'half'))
- gate_grad: bfloat16 [128, 768, 2048], P('expert', 'half')
- up_grad: bfloat16 [128, 768, 2048], P('expert', 'half')
- down_grad: bfloat16 [128, 768, 2048], P('expert', 'half')
The draws below stay inside these ranges and needn't reach their ends.
Inputs may be any that keep to these rules, and one draw needn't show every extreme that they name: `assign`: each row names 8 different experts. Within each aligned block of 128 rows (the rows of one index of expert) no expert is named more than 12 times, and in every draw some expert is named exactly 12 times in some block.
All inputs are finite; a program needn't handle non-finite values.
Results may differ from the reference program's by a relative error of at most 0.011.
Values may be sent and summed in bfloat16 or wider, within the bound.
A program may use at most 128 MiB of HBM per device.

```python
import math
import jax
import jax.numpy as jnp
import numpy as np
from jax import lax

D = 2048
FF = 768
TOP = 8
TOK_DEV = 128
EXPERTS = 128
CAP = 12
TOKENS = 8192
N_EXPERT = 64
N_HALF = 4


def levels(own_key, shape, cuts, smallest, high):
    loudness, own = 1.0, jax.random.fold_in(own_key, 6)
    for axis_at, shards_of in cuts:
        heights = jnp.exp(jax.random.uniform(jax.random.fold_in(own, axis_at), (shards_of,), jnp.float32, smallest / len(cuts), high / len(cuts)))
        loudness = loudness * jnp.repeat(heights, shape[axis_at] // shards_of).reshape([-1 if axis == axis_at else 1 for axis in range(len(shape))])
    return loudness


def routed_block(rng, own, number, rows, number_of, top, limit, slope):
    order = jax.random.permutation(rng, number_of)
    packed, common = load_shares(number_of, rows * top, limit, slope, True), load_shares(number_of, rows * top, limit, slope, False)
    places = jnp.arange(number_of)

    def named(tallies, offset_by):
        used = int((tallies > 0).sum())
        fixed = max(1, used // 4)
        shifted = fixed + (places - fixed + offset_by * (used - fixed)) % max(1, number_of - fixed)
        return jnp.zeros((number_of,), jnp.int32).at[order[jnp.where(places < fixed, places, shifted)]].set(jnp.asarray(tallies, jnp.int32))

    tallies = jnp.where(number % 4 == 0, named(packed, number // 4), named(common, number - number // 4 - 1))
    mixed = jax.random.permutation(jax.random.fold_in(own, 3), number_of)
    giver, taker = mixed[0:number_of // 2 * 2:2], mixed[1:number_of // 2 * 2:2]
    margin = jnp.minimum(tallies[giver] - 1, limit - tallies[taker]) // 2
    margin = jnp.where((giver == order[0]) | (taker == order[0]) | (tallies[taker] == 0), 0, jnp.maximum(margin, 0))
    shifted = jax.random.randint(jax.random.fold_in(own, 4), (number_of // 2,), 0, 1 << 20) % (margin + 1)
    tallies = tallies.at[giver].add(-shifted).at[taker].add(shifted)
    items = jnp.searchsorted(jnp.cumsum(tallies), jnp.arange(rows * top), side="right").astype(jnp.int32)
    grid = items.reshape(top, rows).T
    grid = grid[jax.random.permutation(jax.random.fold_in(own, 1), rows)]
    offset_by = jax.random.randint(jax.random.fold_in(own, 2), (rows, 1), 0, top)
    return jnp.take_along_axis(grid, (jnp.arange(top)[None, :] + offset_by) % top, axis=1)


def load_shares(number_of, total, reach, skew, full):
    loads = [(1 << 20) // math.isqrt(grade ** skew) + 1 for grade in range(1, number_of + 1)]
    largest = reach if full else min(reach, max(-(-total // number_of), total * loads[0] // sum(loads)))
    least = 1 if total - largest >= number_of - 1 else 0
    given, surplus = [largest] + [least] * (number_of - 1), total - largest - least * (number_of - 1)
    while surplus > 0:
        movable = [i for i in range(1, number_of) if given[i] < largest] or [i for i in range(1, number_of) if given[i] < reach]
        mass, budget = sum([loads[i] for i in movable]), surplus
        for i in movable:
            addition = min(reach - given[i], max(1, budget * loads[i] // mass), surplus)
            given[i] = given[i] + addition
            surplus = surplus - addition
    return np.array(given)


def noise(rng, extent, deviation, reach, cuts=(), kind=jnp.bfloat16):
    array = jax.random.normal(rng, extent, jnp.float32) * deviation
    if len(cuts) > 0:
        array = levels(rng, extent, cuts, -0.22, 0.18) * array
    return jnp.clip(array, min=-reach, max=reach).astype(kind)


def setup_inputs(seed: int = 0) -> dict:
    arg_keys = jax.random.split(jax.random.key(seed), 8)
    tokens = noise(arg_keys[0], (TOKENS, D), 1.0, 6.0, ((0, 64),))
    out_grad = noise(arg_keys[1], (TOKENS, D), 1.0, 6.0, ((0, 64),))
    assign_keys = jax.random.split(jax.random.fold_in(arg_keys[2], 1), TOKENS // TOK_DEV)
    assign_turns = jax.random.permutation(jax.random.fold_in(arg_keys[2], 3), TOKENS // TOK_DEV)
    assign = jax.vmap(lambda own, number: routed_block(jax.random.fold_in(arg_keys[2], 2), own, number, TOK_DEV, EXPERTS, TOP, CAP, 2))(assign_keys, assign_turns).reshape((TOKENS, TOP))
    gate_weights = jnp.clip(0.099609375 + 0.9003906 * jax.random.uniform(arg_keys[3], (TOKENS, TOP), jnp.float32) ** levels(arg_keys[3], (TOKENS, TOP), ((0, 64),), -0.2, 0.2), 0.099609375, 1.0).astype(jnp.bfloat16)
    w_gate = noise(arg_keys[4], (EXPERTS, FF, D), D ** -0.5, 0.125, ((0, 64), (1, 4)))
    w_up = noise(arg_keys[5], (EXPERTS, FF, D), D ** -0.5, 0.125, ((0, 64), (1, 4)))
    w_down = noise(arg_keys[6], (EXPERTS, FF, D), FF ** -0.5, 0.21875, ((0, 64), (1, 4)))
    return {"tokens": tokens, "out_grad": out_grad, "assign": assign, "gate_weights": gate_weights, "w_gate": w_gate, "w_up": w_up, "w_down": w_down}


def expert_pass(rows_in, scaled, weight_gate, weight_up, weight_down):
    quarter = FF // N_HALF
    dims = (((1,), (1,)), ((), ()))
    first = (((0,), (0,)), ((), ()))
    term_sum = jnp.zeros((rows_in.shape[0], D), jnp.float32)
    gate_parts = []
    up_parts = []
    down_parts = []
    for index in range(N_HALF):
        wg_part = weight_gate[index * quarter:(index + 1) * quarter]
        wu_part = weight_up[index * quarter:(index + 1) * quarter]
        wd_part = weight_down[index * quarter:(index + 1) * quarter]
        gate_pre = lax.dot_general(rows_in, wg_part, dims, preferred_element_type=jnp.float32)
        up_pre = lax.dot_general(rows_in, wu_part, dims, preferred_element_type=jnp.float32)
        sig = jax.nn.sigmoid(gate_pre)
        silu_gate = gate_pre * sig
        hidden = (silu_gate * up_pre).astype(jnp.bfloat16)
        hidden_grad = lax.dot_general(scaled, wd_part, dims, preferred_element_type=jnp.float32)
        gate_pre_grad = (hidden_grad * up_pre * (sig * (1.0 + gate_pre * (1.0 - sig)))).astype(jnp.bfloat16)
        up_pre_grad = (hidden_grad * silu_gate).astype(jnp.bfloat16)
        down_parts.append(lax.dot_general(hidden, scaled, first, preferred_element_type=jnp.float32).astype(jnp.bfloat16))
        gate_parts.append(lax.dot_general(gate_pre_grad, rows_in, first, preferred_element_type=jnp.float32).astype(jnp.bfloat16))
        up_parts.append(lax.dot_general(up_pre_grad, rows_in, first, preferred_element_type=jnp.float32).astype(jnp.bfloat16))
        term = jnp.dot(gate_pre_grad, wg_part, preferred_element_type=jnp.float32)
        term = term + jnp.dot(up_pre_grad, wu_part, preferred_element_type=jnp.float32)
        term_sum = term_sum + term.astype(jnp.bfloat16).astype(jnp.float32)
    return (jnp.concatenate(gate_parts, 0), jnp.concatenate(up_parts, 0), jnp.concatenate(down_parts, 0), term_sum)


def reference(tokens, out_grad, assign, gate_weights, w_gate, w_up, w_down):
    pairs = TOKENS * TOP
    flat = assign.reshape(N_EXPERT, TOK_DEV * TOP)
    onehot = (flat[:, :, None] == jnp.arange(EXPERTS, dtype=jnp.int32)[None, None, :]).astype(jnp.int32)
    position = jnp.sum(jnp.cumsum(onehot, axis=1) * onehot, axis=2) - 1
    block_ids = jnp.arange(N_EXPERT, dtype=jnp.int32)[:, None]
    slot_ids = (flat * (N_EXPERT * CAP) + block_ids * CAP + position).reshape(-1).astype(jnp.int32)
    total = EXPERTS * N_EXPERT * CAP
    filler = jnp.full((total,), pairs, jnp.int32).at[slot_ids].set(jnp.arange(pairs, dtype=jnp.int32))
    filler = filler.reshape(EXPERTS, N_EXPERT * CAP)
    gate_flat = gate_weights.reshape(-1)

    def one_expert(inputs):
        fill_ids, weight_gate, weight_up, weight_down = inputs
        token_of = fill_ids // TOP
        rows_in = jnp.take(tokens, token_of, axis=0, mode="fill", fill_value=0)
        grad_rows = jnp.take(out_grad, token_of, axis=0, mode="fill", fill_value=0)
        gate_slot = jnp.take(gate_flat, fill_ids, axis=0, mode="fill", fill_value=0)
        scaled = (gate_slot.astype(jnp.float32)[:, None] * grad_rows.astype(jnp.float32)).astype(jnp.bfloat16)
        return expert_pass(rows_in, scaled, weight_gate, weight_up, weight_down)

    gate_grad, up_grad, down_grad, terms = lax.map(one_expert, (filler, w_gate, w_up, w_down))
    per_pair = jnp.take(terms.reshape(total, D), slot_ids, axis=0)
    input_grad = jnp.sum(per_pair.reshape(TOKENS, TOP, D), axis=1).astype(jnp.bfloat16)
    return input_grad, gate_grad, up_grad, down_grad
```

```python
import jax
import jax.numpy as jnp
from jax import lax
from jax.experimental import pallas as pl
from jax.experimental.pallas import tpu as pltpu
from jax.sharding import PartitionSpec as P

CAP = 12
ROWS = 8


def row_tables(slots_total):
    row = jnp.arange(slots_total, dtype=jnp.int32)
    owner, inner = row // (2 * CAP), row % (2 * CAP)
    group, place = inner // ROWS, inner % ROWS
    second = (group == 2) | ((group == 1) & (place >= 4))
    expert = owner * 2 + second.astype(jnp.int32)
    slot = jnp.where(group == 1, 8 + place % 4, place)
    return expert, slot


def routing(assign, gate_weights, experts, slots_total):
    tok_rows = assign.shape[0]
    hit = assign[:, :, None] == jnp.arange(experts, dtype=jnp.int32)[None, None, :]
    named = jnp.any(hit, axis=1)
    weight = jnp.sum(jnp.where(hit, gate_weights[:, :, None].astype(jnp.float32), 0.0), axis=1)
    earlier = jnp.tril(jnp.ones((tok_rows, tok_rows), jnp.bfloat16), -1)
    position = jnp.dot(earlier, named.astype(jnp.bfloat16), preferred_element_type=jnp.float32)
    position = jnp.where(named, position, -1.0).astype(jnp.bfloat16)
    expert, slot = row_tables(slots_total)
    pick = (expert[:, None] == jnp.arange(experts, dtype=jnp.int32)[None, :]).astype(jnp.bfloat16)
    dims = (((1,), (1,)), ((), ()))
    placed = lax.dot_general(pick, position, dims, preferred_element_type=jnp.float32)
    weights = lax.dot_general(
        pick, weight.astype(jnp.bfloat16), dims, preferred_element_type=jnp.float32
    )
    chosen = placed == slot.astype(jnp.float32)[:, None]
    return chosen.astype(jnp.bfloat16), jnp.where(chosen, weights, 0.0).astype(jnp.bfloat16)


def expert_math(rows, scaled, w_gate, w_up, w_down):
    total, width = rows.shape
    half = total // 3
    dims = (((1,), (1,)), ((), ()))
    first = (((0,), (0,)), ((), ()))
    place = lax.broadcasted_iota(jnp.int32, (2 * half, 1), 0)
    grads = []
    terms = []
    for expert in range(2):
        low = expert * half
        x = rows[low : low + 2 * half]
        s = scaled[low : low + 2 * half]
        if expert == 0:
            mine = (place < half) | (place % ROWS < 4)
        else:
            mine = (place >= half) | (place % ROWS >= 4)
        gate_pre = lax.dot_general(x, w_gate[expert], dims, preferred_element_type=jnp.float32)
        up_pre = lax.dot_general(x, w_up[expert], dims, preferred_element_type=jnp.float32)
        hidden_grad = lax.dot_general(s, w_down[expert], dims, preferred_element_type=jnp.float32)
        sig = jax.nn.sigmoid(gate_pre)
        silu = gate_pre * sig
        hidden = jnp.where(mine, silu * up_pre, 0.0).astype(jnp.bfloat16)
        gate_back = jnp.where(
            mine, hidden_grad * up_pre * (sig * (1.0 + gate_pre * (1.0 - sig))), 0.0
        ).astype(jnp.bfloat16)
        up_back = jnp.where(mine, hidden_grad * silu, 0.0).astype(jnp.bfloat16)
        grads.append(
            tuple(
                lax.dot_general(a, b, first, preferred_element_type=jnp.float32).astype(jnp.bfloat16)
                for a, b in ((gate_back, x), (up_back, x), (hidden, s))
            )
        )
        term = jnp.dot(gate_back, w_gate[expert], preferred_element_type=jnp.float32)
        terms.append(term + jnp.dot(up_back, w_up[expert], preferred_element_type=jnp.float32))
    slot_terms = jnp.concatenate(
        [terms[0][:half], terms[0][half:] + terms[1][:half], terms[1][half:]], axis=0
    ).astype(jnp.bfloat16)
    gate_grad, up_grad, down_grad = (jnp.stack(pair, 0) for pair in zip(*grads))
    return slot_terms, gate_grad, up_grad, down_grad


MESH = pl.DeviceIdType.MESH
NX = 4
NZ = 8
OWNERS = 64
HALVES = 4


def position():
    e = lax.axis_index("expert")
    y = lax.axis_index("half")
    return e, y, e // 16, (e % 16) // 2, e % 2


def peer(e, y):
    return {"expert": e, "half": y}


def distance(k):
    return ((k + 1) // 2) * (1 - 2 * ((k + 1) % 2))


def member(x, zed, core, j):
    return ((x + j // 2) % NX) * 16 + zed * 2 + (core + j) % 2


def greet(e, y, above, below):
    barrier = pltpu.get_barrier_semaphore()

    def hello(i, carry):
        pl.semaphore_signal(
            barrier, inc=1, device_id=peer((e + i) % OWNERS, y), device_id_type=MESH
        )
        return carry

    lax.fori_loop(1, OWNERS, hello, 0)
    for other in (above, below):
        pl.semaphore_signal(barrier, inc=1, device_id=peer(e, other), device_id_type=MESH)
    pl.semaphore_wait(barrier, OWNERS + 1)


def remote(src, dst, send, recv, to):
    return pltpu.make_async_remote_copy(
        src_ref=src, dst_ref=dst, send_sem=send, recv_sem=recv, device_id=to, device_id_type=MESH
    )


def dispatch_kernel(
    sent0, sent1, out0, out1, send_sem, recv_sem, fsend, frecv, rsend, rrecv, local_sem
):
    e, y, x, z, core = position()
    above, below, across = (y + 1) % HALVES, (y + 3) % HALVES, (y + 2) % HALVES
    part = sent0.shape[-1]
    sents, outs = (sent0, sent1), (out0, out1)

    def cols(group):
        return pl.ds(pl.multiple_of(group * part, part), part)

    greet(e, y, above, below)

    def chunk(a, k, j):
        dest = member(x, (z + distance(k) + NZ) % NZ, core, j)
        return dest, remote(
            sents[a].at[dest],
            outs[a].at[:, x, e % 16, :, cols(y)],
            send_sem.at[a, dest],
            recv_sem.at[a, e],
            peer(dest, y),
        )

    def over_chunks(a, act):
        def outer(k, carry):
            def inner(j, carry):
                dest, copy = chunk(a, k, j)

                @pl.when(dest != e)
                def _():
                    act(copy)

                return carry

            return lax.fori_loop(0, 8, inner, carry)

        lax.fori_loop(0, NZ, outer, 0)

    own = [
        pltpu.make_async_copy(
            sents[a].at[e], outs[a].at[:, x, e % 16, :, cols(y)], local_sem.at[a]
        )
        for a in range(2)
    ]
    for a in range(2):
        own[a].start()
        over_chunks(a, lambda copy: copy.start())

    def source(k):
        return (z - distance(k) + NZ) % NZ

    def block(a, k, group):
        return outs[a].at[:, :, pl.ds(source(k) * 2, 2), :, cols(group)]

    def lower(a, k, group):
        return outs[a].at[:, pl.ds(0, 2), pl.ds(source(k) * 2, 2), :, cols(group)]

    def upper(a, k, group):
        return outs[a].at[:, pl.ds(2, 2), pl.ds(source(k) * 2, 2), :, cols(group)]

    def move(ref, send, recv, i, a, k, to):
        return remote(ref, ref, send.at[i, a, k], recv.at[i, a, k], peer(e, to))

    def forward(a, k):
        def arrive(j, carry):
            src = member(x, source(k), core, j)

            @pl.when(src != e)
            def _():
                remote(
                    sents[a].at[src],
                    outs[a].at[:, src // 16, src % 16, :, cols(y)],
                    send_sem.at[a, src],
                    recv_sem.at[a, src],
                    peer(src, y),
                ).wait_recv()

            return carry

        lax.fori_loop(0, 8, arrive, 0)
        move(block(a, k, y), fsend, frecv, 0, a, k, above).start()
        move(block(a, k, y), fsend, frecv, 1, a, k, below).start()

    def relay(a, k):
        move(block(a, k, below), fsend, frecv, 0, a, k, above).wait_recv()
        move(lower(a, k, below), rsend, rrecv, 0, a, k, above).start()
        move(block(a, k, above), fsend, frecv, 1, a, k, below).wait_recv()
        move(upper(a, k, above), rsend, rrecv, 1, a, k, below).start()

    def steps(a):
        def step(k, carry):
            forward(a, k)
            relay(a, k - 1)
            return carry

        lax.fori_loop(1, NZ, step, 0)

    for a in range(2):
        own[a].wait()
        forward(a, 0)
        if a == 1:
            relay(0, NZ - 1)
        steps(a)
    relay(1, NZ - 1)

    for a in range(2):

        def finish(k, carry, a=a):
            move(lower(a, k, across), rsend, rrecv, 0, a, k, above).wait_recv()
            move(upper(a, k, across), rsend, rrecv, 1, a, k, below).wait_recv()
            move(block(a, k, y), fsend, frecv, 0, a, k, above).wait_send()
            move(block(a, k, y), fsend, frecv, 1, a, k, below).wait_send()
            move(lower(a, k, below), rsend, rrecv, 0, a, k, above).wait_send()
            move(upper(a, k, above), rsend, rrecv, 1, a, k, below).wait_send()
            return carry

        lax.fori_loop(0, NZ, finish, 0)
        over_chunks(a, lambda copy: copy.wait_send())


def dispatch(sent0, sent1):
    part = sent0.shape[-1]
    full = jax.ShapeDtypeStruct((3, NX, 16, ROWS, part * HALVES), jnp.bfloat16)
    dma = pltpu.SemaphoreType.DMA
    return pl.pallas_call(
        dispatch_kernel,
        out_shape=(full, full),
        in_specs=[pl.BlockSpec(memory_space=pltpu.VMEM)] * 2,
        out_specs=(pl.BlockSpec(memory_space=pl.ANY),) * 2,
        scratch_shapes=[
            dma((2, OWNERS)),
            dma((2, OWNERS)),
            dma((2, 2, NZ)),
            dma((2, 2, NZ)),
            dma((2, 2, NZ)),
            dma((2, 2, NZ)),
            dma((2,)),
        ],
        compiler_params=pltpu.CompilerParams(
            collective_id=0, has_side_effects=True, vmem_limit_bytes=48 << 20
        ),
        name="dispatch",
    )(sent0, sent1)


def combine_kernel(
    terms, back, low_in, high_in, low_out, high_out, from_below, from_above, total,
    ssend, srecv, send_sem, recv_sem, local_sem,
):
    e, y, x, z, core = position()
    above, below, across = (y + 1) % HALVES, (y + 3) % HALVES, (y + 2) % HALVES
    part = back.shape[-1]

    def cols(group):
        return pl.ds(pl.multiple_of(group * part, part), part)

    def zed(n):
        return (z + distance(NZ - 1 - n) + NZ) % NZ

    def pair(n):
        return pl.ds(zed(n) * 2, 2)

    lows, highs = pl.ds(0, 2), pl.ds(2, 2)
    greet(e, y, above, below)

    def moves(n, i):
        src, dst, to = (
            lambda: (terms.at[:, lows, pair(n), :, cols(across)], low_in.at[n], above),
            lambda: (terms.at[:, highs, pair(n), :, cols(across)], high_in.at[n], below),
            lambda: (terms.at[:, highs, pair(n), :, cols(above)], from_below.at[n, :, highs], above),
            lambda: (terms.at[:, lows, pair(n), :, cols(below)], from_above.at[n, :, lows], below),
            lambda: (low_out.at[n], from_below.at[n, :, lows], above),
            lambda: (high_out.at[n], from_above.at[n, :, highs], below),
        )[i]()
        return remote(src, dst, ssend.at[i, n], srecv.at[i, n], peer(e, to))

    def first(n):
        for i in range(4):
            moves(n, i).start()

    def second(n):
        f32 = jnp.float32
        moves(n, 0).wait_recv()
        own = terms[:, lows, pair(n), :, cols(above)]
        low_out[n] = (low_in[n].astype(f32) + own.astype(f32)).astype(jnp.bfloat16)
        moves(n, 4).start()
        moves(n, 1).wait_recv()
        own = terms[:, highs, pair(n), :, cols(below)]
        high_out[n] = (high_in[n].astype(f32) + own.astype(f32)).astype(jnp.bfloat16)
        moves(n, 5).start()

    def home(n, j):
        dest = member(x, zed(n), core, j)
        return dest, remote(
            total.at[n, :, dest // 16, dest % 2],
            back.at[e],
            send_sem.at[dest],
            recv_sem.at[e],
            peer(dest, y),
        )

    def third(n):
        f32 = jnp.float32
        for i in range(2, 6):
            moves(n, i).wait_recv()
        own = terms[:, :, pair(n), :, cols(y)]
        total[n] = (
            own.astype(f32) + from_below[n].astype(f32) + from_above[n].astype(f32)
        ).astype(jnp.bfloat16)

        def deliver(j, carry):
            dest, copy = home(n, j)

            @pl.when(dest != e)
            def _():
                copy.start()

            return carry

        lax.fori_loop(0, 8, deliver, 0)

    first(0)
    first(1)
    second(0)

    def step(n, carry):
        first(n)
        second(n - 1)
        third(n - 2)
        return carry

    lax.fori_loop(2, NZ, step, 0)
    second(NZ - 1)
    third(NZ - 2)
    third(NZ - 1)
    own = pltpu.make_async_copy(total.at[NZ - 1, :, x, core], back.at[e], local_sem)
    own.start()

    def finish(n, carry):
        for i in range(6):
            moves(n, i).wait_send()

        def settle(j, carry):
            dest, copy = home(n, j)

            @pl.when(dest != e)
            def _():
                copy.wait_send()
                remote(
                    total.at[n, :, dest // 16, dest % 2],
                    back.at[dest],
                    send_sem.at[dest],
                    recv_sem.at[dest],
                    peer(dest, y),
                ).wait_recv()

            return carry

        return lax.fori_loop(0, 8, settle, carry)

    lax.fori_loop(0, NZ, finish, 0)
    own.wait()


def combine(terms):
    part = terms.shape[-1] // HALVES
    bf16 = jnp.bfloat16
    dma = pltpu.SemaphoreType.DMA
    half = pltpu.VMEM((NZ, 3, 2, 2, ROWS, part), bf16)
    full = pltpu.VMEM((NZ, 3, NX, 2, ROWS, part), bf16)
    return pl.pallas_call(
        combine_kernel,
        out_shape=jax.ShapeDtypeStruct((OWNERS, 3, ROWS, part), bf16),
        in_specs=[pl.BlockSpec(memory_space=pltpu.VMEM)],
        out_specs=pl.BlockSpec(memory_space=pl.ANY),
        scratch_shapes=[
            half, half, half, half, full, full, full,
            dma((6, NZ)), dma((6, NZ)), dma((OWNERS,)), dma((OWNERS,)), dma,
        ],
        compiler_params=pltpu.CompilerParams(
            collective_id=1, has_side_effects=True, vmem_limit_bytes=48 << 20
        ),
        name="combine",
    )(terms)


def on_device(tokens, out_grad, assign, gate_weights, w_gate, w_up, w_down):
    tok_rows, width = tokens.shape
    mine = lax.axis_index("half")
    experts = OWNERS * w_gate.shape[0]
    total = experts * CAP
    part = width // HALVES
    chosen, weighted = routing(assign, gate_weights, experts, total)

    def pack(matrix, source):
        cols = lax.dynamic_slice(source, (0, mine * part), (tok_rows, part))
        sent = jnp.dot(matrix, cols, preferred_element_type=jnp.float32).astype(jnp.bfloat16)
        return sent.reshape(OWNERS, 3, ROWS, part)

    rows, scaled = dispatch(pack(chosen, tokens), pack(weighted, out_grad))
    slot_terms, gate_grad, up_grad, down_grad = expert_math(
        rows.reshape(total, width), scaled.reshape(total, width), w_gate, w_up, w_down
    )
    returned = combine(slot_terms.reshape(3, NX, 16, ROWS, width))
    combined = lax.dot_general(
        chosen,
        returned.reshape(total, part),
        (((0,), (0,)), ((), ())),
        preferred_element_type=jnp.float32,
    ).astype(jnp.bfloat16)
    combined = lax.all_to_all(combined, "half", split_axis=0, concat_axis=1, tiled=True)
    return combined, gate_grad, up_grad, down_grad


def solution(mesh):
    in_specs = (
        P("expert", None),
        P("expert", None),
        P("expert", None),
        P("expert", None),
        P("expert", "half", None),
        P("expert", "half", None),
        P("expert", "half", None),
    )
    out_specs = (
        P(("expert", "half"), None),
        P("expert", "half", None),
        P("expert", "half", None),
        P("expert", "half", None),
    )
    return jax.shard_map(
        on_device, mesh=mesh, in_specs=in_specs, out_specs=out_specs, check_vma=False
    )
```
